32 devices in a mesh: group: 4 (over x, core), member: 8 (over z, y).
Axes of the slice: x: 2, y: 2, z: 4, core: 2. Of those that a mesh axis runs over, the one named last changes fastest.
Arguments:
- amplitudes: bfloat16 [128, 512, 128], P(('group', 'member')), may hold values from -6 to 6
- integrals: bfloat16 [7168, 128, 128], P(('group', 'member')), may hold values from -0.0625 to 0.0625
- task_plan: int32 [7168, 3], P(('group', 'member')), may hold values from 0 to 127, as said below
Outputs:
- residual_tiles: float32 [128, 512, 128], P(('group', 'member'))
The draws below stay inside these ranges and needn't reach their ends.
Inputs may be any that keep to these rules, and one draw needn't show every extreme that they name: `task_plan`: column 0 is the source tile, column 1 the destination tile, column 2 the executing device as index in the order group, then member. Both tiles of a row lie in the same symmetry block of 32 consecutive tiles, and the executor is a device of the group that holds that block. Every device is the executor of exactly 224 rows. The rows of one device name one executor at most 7 times, and name destination tiles held by one device at most 14 times; both bounds are reached in every draw.
All inputs are finite; a program needn't handle non-finite values.
Results may differ from the reference program's by a relative error of at most 0.0003.
Values may be sent and summed in bfloat16 or wider, within the bound.
No kernel may reach another device: no remote copies, remote signals or barrier semaphores. Data moves between devices by JAX's collectives and lax.ppermute only.
A program may use at most 192 MiB of HBM per device.

```python
import math
import jax
import jax.numpy as jnp
from jax import lax

W = 128
ROWS = 512
TILE_DEV = 4
TASK_DEV = 224
NTILE = 128
NTASK = 7168
N_GROUP = 4
N_MEMBER = 8


def draw_task_plan(key, part):
    devices_all = N_GROUP * N_MEMBER
    base = TASK_DEV // devices_all
    extra = TASK_DEV - base * devices_all
    peer_most = (TASK_DEV + devices_all - 1) // devices_all
    dest_most = 2 * peer_most
    keys = jax.random.split(jax.random.fold_in(key, 41), 7)
    first_perm = jax.random.permutation(keys[0], devices_all).astype(jnp.int32)
    second_perm = jax.random.permutation(keys[1], devices_all).astype(jnp.int32)
    senders = jnp.arange(devices_all, dtype=jnp.int32)
    counts = base + ((first_perm[None, :] - second_perm[:, None]) % devices_all < extra).astype(jnp.int32)
    slots = devices_all * peer_most
    copies = jnp.arange(slots, dtype=jnp.int32) % peer_most
    slot_exec = jnp.arange(slots, dtype=jnp.int32) // peer_most
    used = copies[None, :] < counts[:, slot_exec]
    noise = jax.random.randint(keys[2], (devices_all, slots), 0, 1 << 20, dtype=jnp.int32)
    score = (noise + jnp.where(used, 0, 1 << 20)) * slots + jnp.arange(slots, dtype=jnp.int32)[None, :]
    chosen = jnp.argsort(score, axis=1)[:, :TASK_DEV].astype(jnp.int32)
    executor = chosen // peer_most
    sym_block = executor // N_MEMBER
    onehot = (sym_block[:, :, None] == jnp.arange(N_GROUP, dtype=jnp.int32)[None, None, :]).astype(jnp.int32)
    rank = jnp.sum(jnp.cumsum(onehot, axis=1) * onehot, axis=2) - 1
    hot_member = jax.random.randint(keys[3], (N_GROUP,), 0, N_MEMBER, dtype=jnp.int32)
    member_ids = jnp.arange(N_MEMBER, dtype=jnp.int32)
    mixed = jax.random.randint(keys[4], (devices_all, N_GROUP, N_MEMBER), 0, 1 << 20, dtype=jnp.int32) * N_MEMBER + member_ids[None, None, :]
    mixed = jnp.where(member_ids[None, None, :] == hot_member[None, :, None], 1 << 30, mixed)
    others = jnp.argsort(mixed, axis=2).astype(jnp.int32)
    later = jnp.maximum(rank - dest_most, 0) % (N_MEMBER - 1)
    other_owner = others[senders[:, None], sym_block, later]
    owner = jnp.where(rank < dest_most, hot_member[sym_block], other_owner)
    within = jax.random.randint(keys[5], (devices_all, TASK_DEV), 0, TILE_DEV, dtype=jnp.int32)
    destination = (sym_block * N_MEMBER + owner) * TILE_DEV + within
    source = sym_block * (TILE_DEV * N_MEMBER) + jax.random.randint(keys[6], (devices_all, TASK_DEV), 0, TILE_DEV * N_MEMBER, dtype=jnp.int32)
    return jnp.stack([source, destination, executor], axis=-1).reshape(devices_all * TASK_DEV, 3).astype(jnp.int32)


def block_levels(own_key, dims, cuts, smallest, largest):
    loudness, own = 1.0, jax.random.fold_in(own_key, 6)
    for position, shards_of in cuts:
        heights = jnp.exp(jax.random.uniform(jax.random.fold_in(own, position), (shards_of,), jnp.float32, smallest / len(cuts), largest / len(cuts)))
        loudness = loudness * jnp.repeat(heights, dims[position] // shards_of).reshape([-1 if axis == position else 1 for axis in range(len(dims))])
    return loudness


def normal_values(stream_key, dims, spread, reach, cuts=(), kind=jnp.bfloat16):
    result = spread * jax.random.normal(stream_key, dims, jnp.float32)
    if cuts:
        result = result * block_levels(stream_key, dims, cuts, -0.22, 0.18)
    return jnp.clip(result, -reach, reach).astype(kind)


def setup_inputs(seed: int = 0) -> dict:
    key_list = jax.random.split(jax.random.key(seed), 4)
    amplitudes = normal_values(key_list[0], (NTILE, ROWS, W), 1.0, 6.0, ((0, 32),))
    integrals = normal_values(key_list[1], (NTASK, W, W), (W * TASK_DEV // TILE_DEV) ** -0.5, 0.0625, ((0, 32),))
    task_plan = draw_task_plan(jax.random.fold_in(key_list[3], 71), 0)
    return dict(amplitudes=amplitudes, integrals=integrals, task_plan=task_plan)


def reference(amplitudes, integrals, task_plan):
    count = integrals.shape[0]
    block = math.gcd(count, 256)
    turns = count // block
    width = integrals.shape[-1]
    rows = amplitudes.shape[1]
    source = task_plan[:, 0].reshape(turns, block)
    target = task_plan[:, 1].reshape(turns, block)
    tiles = integrals.reshape(turns, block, width, width)

    def advance(total, pieces):
        piece_tiles, piece_source, piece_target = pieces
        left_rows = jnp.take(amplitudes, piece_source, axis=0).astype(jnp.float32)
        product = jnp.einsum("brw,bwv->brv", left_rows, piece_tiles.astype(jnp.float32),
                             precision=lax.Precision.HIGHEST)
        return total.at[piece_target].add(product), None

    start_total = jnp.zeros((amplitudes.shape[0], rows, width), jnp.float32)
    total, unused = lax.scan(advance, start_total, (tiles, source, target))
    return total
```

```python
import functools

import jax
import jax.numpy as jnp
from jax import lax
from jax.experimental import pallas as pl
from jax.experimental.pallas import tpu as pltpu
from jax.sharding import PartitionSpec as P


PARTS = (3, 3, 2)
STEPS = 4.0
LEVELS = 32000.0
SMALLEST = 2.0**-110

SMEM = pl.BlockSpec(memory_space=pltpu.SMEM)
VMEM = pl.BlockSpec(memory_space=pltpu.VMEM)
ANY = pl.BlockSpec(memory_space=pl.ANY)


def params(name):
    return dict(compiler_params=pltpu.CompilerParams(vmem_limit_bytes=60 << 20), name=name)


def cost(flops, size):
    return pl.CostEstimate(flops=flops, bytes_accessed=size, transcendentals=0)


def pad16(count):
    return (count + 15) // 16 * 16


def encode(values, into, at, scales, row):
    peak = jnp.maximum(jnp.max(jnp.abs(values), axis=0, keepdims=True), SMALLEST)
    level = jnp.ceil(jnp.log2(peak) * STEPS)
    scales[pl.ds(row, 1), :] = level
    codes = jnp.round(values * (jnp.exp2(level * (-1.0 / STEPS)) * LEVELS))
    into[pl.ds(at, values.shape[0]), :] = codes.astype(jnp.int32).astype(jnp.int16)


def unit(level):
    return jnp.exp2(level * (1.0 / STEPS)) * (1.0 / LEVELS)


def decode(codes, at, rows, scale):
    return codes[pl.ds(at, rows), :].astype(jnp.int32).astype(jnp.float32) * scale


def sort_body(groups, members, tile_grp, cap, width, plan, tiles, order, labels, first, held, count, sem):
    tasks = tiles.shape[0]
    copy = pltpu.make_async_copy(tiles, held, sem)
    copy.start()
    mine = lax.axis_index("group")
    for k in range(groups):
        count[k] = 0
    if groups * cap > tasks:

        def clear(j, carry):
            for k in range(groups):
                order[k * cap + j] = -1
                labels[k, 0, j] = 0
                labels[k, 1, j] = 0
            return carry

        lax.fori_loop(0, cap, clear, 0)

    def assign(i, carry):
        k = (plan[2, i] // members) ^ mine
        at = count[k]
        count[k] = at + 1
        order[k * cap + at] = i
        labels[k, 0, at] = plan[0, i] % tile_grp
        labels[k, 1, at] = plan[1, i] % tile_grp
        return carry

    lax.fori_loop(0, tasks, assign, 0, unroll=4)
    copy.wait()
    pack(groups, cap, 0, [width], order, held, first)


def pack(groups, cap, low, widths, order, held, outs):
    tasks = held.shape[0]
    unroll = 4 if cap % 4 == 0 else 1

    def step(j, carry):
        for k in range(groups):
            for u in range(unroll):
                at = j * unroll + u
                i = order[k * cap + at]
                if groups * cap > tasks:
                    tile = held[jnp.maximum(i, 0)]
                    tile = jnp.where(i >= 0, tile, jnp.zeros_like(tile))
                else:
                    tile = held[i]
                turned = tile[:, low : low + sum(widths)].T
                start = 0
                for c, width in enumerate(widths):
                    outs[c * groups + k][at] = turned[start : start + width]
                    start += width
        return carry

    lax.fori_loop(0, cap // unroll, step, 0)


def first_body(groups, members, tile_grp, cap, width, plan, tiles, order, labels, *rest):
    sort_body(groups, members, tile_grp, cap, width, plan, tiles, order, labels, rest[:groups], *rest[groups:])


def rest_body(groups, cap, low, widths, order, tiles, *outs):
    pack(groups, cap, low, widths, order, tiles, outs)


def contract_body(groups, members, tile_dev, *refs):
    labels, refs = refs[:groups], refs[groups:]
    pieces, refs = refs[:groups], refs[groups:]
    blocks, refs = refs[:members], refs[members:]
    keep, send, held, total, scales, sems = refs[-6:]
    cap, width, _ = pieces[0].shape
    copies = [
        pltpu.make_async_copy(block, held.at[pl.ds(r * tile_dev, tile_dev)], sems.at[r])
        for r, block in enumerate(blocks)
    ]
    for copy in copies:
        copy.start()
    me = lax.axis_index("member")
    total[...] = jnp.zeros_like(total)
    for copy in copies:
        copy.wait()
    unroll = 2 if cap % 2 == 0 else 1

    def step(j, carry):
        found = []
        for u in range(unroll):
            for k in range(groups):
                at = j * unroll + u
                source = labels[k][0, at] ^ (me * tile_dev)
                product = jnp.dot(pieces[k][at], held[source], preferred_element_type=jnp.float32)
                found.append((labels[k][1, at], product))
        for dest, product in found:
            total[dest] += product
        return carry

    lax.fori_loop(0, cap // unroll, step, 0)
    low = me % 2

    def hand(i, carry):
        outer, t = i // tile_dev, i % tile_dev
        stay = (outer * 2 + low) * tile_dev + t
        go = (outer * 2 + 1 - low) * tile_dev + t
        keep[i] = total[stay]
        encode(total[go], send, i * width, scales, i)
        return carry

    count = members // 2 * tile_dev
    scales[...] = jnp.zeros_like(scales)
    lax.fori_loop(0, count, hand, 0)
    send[pl.ds(count * width, scales.shape[0]), :] = scales[...].astype(jnp.int32).astype(jnp.int16)


def middle_body(lines, tile_dev, keep, codes, *refs):
    own, sends, (scales, fresh) = refs[-lines - 2], refs[-lines - 1 : -2], refs[-2:]
    count, width, _ = keep.shape
    scales[...] = codes[pl.ds(count * width, scales.shape[0]), :].astype(jnp.int32).astype(jnp.float32)
    outer = lax.axis_index("member") // 2

    def value(i):
        return keep[i] + decode(codes, i * width, width, unit(scales[pl.ds(i, 1), :]))

    fresh[...] = jnp.zeros_like(fresh)
    for k in range(lines):
        there = outer ^ k
        for t in range(tile_dev):
            i = there * tile_dev + t
            if k == 0:
                own[t] = value(i)
            else:
                encode(value(i), sends[k - 1], t * width, fresh, t)
        if k:
            sends[k - 1][pl.ds(tile_dev * width, fresh.shape[0]), :] = fresh[...].astype(jnp.int32).astype(jnp.int16)


def last_body(chunks, lines, tile_dev, *refs):
    out, scales, sums = refs[-3:]
    low = 0
    for c in range(chunks):
        own, codes = refs[c * lines], refs[c * lines + 1 : (c + 1) * lines]
        width = own.shape[1]
        for k, code in enumerate(codes):
            scales[k] = code[pl.ds(tile_dev * width, scales.shape[1]), :].astype(jnp.int32).astype(jnp.float32)
        for t in range(tile_dev):
            value = own[t]
            for k, code in enumerate(codes):
                value = value + decode(code, t * width, width, unit(scales[k, t : t + 1, :]))
            sums[t, low : low + width, :] = value
        low += width
    for t in range(tile_dev):
        out[t] = sums[t].T


def on_device(amplitudes, integrals, task_plan):
    groups = lax.axis_size("group")
    members = lax.axis_size("member")
    tile_dev, rows, width = amplitudes.shape
    tasks = integrals.shape[0]
    tile_grp = tile_dev * members
    cap = (tasks + groups * members - 1) // (groups * members) * members
    lines = members // 2
    widths = [width // 8 * part for part in PARTS]
    chunks = len(widths)
    bf16, f32, i16, i32 = jnp.bfloat16, jnp.float32, jnp.int16, jnp.int32
    shape = jax.ShapeDtypeStruct

    def swap(x, axis, k):
        size = lax.axis_size(axis)
        return lax.ppermute(x, axis, [(i, i ^ k) for i in range(size)])

    mine = jnp.swapaxes(amplitudes, 1, 2)
    column = [mine]
    for k in range(1, lines):
        near = k & -k
        column.append(swap(column[k - near], "member", 2 * near))
    across = [swap(mine, "member", 1)]
    for k in range(1, lines):
        across.append(swap(column[k], "member", 1))
    blocks = [block for pair in zip(column, across) for block in pair]

    bare = [shape((cap, w, width), bf16) for w in widths]
    outs = pl.pallas_call(
        functools.partial(first_body, groups, members, tile_grp, cap, widths[0]),
        out_shape=[shape((groups * cap,), i32), shape((groups, 2, cap), i32)] + [bare[0]] * groups,
        in_specs=[SMEM, ANY],
        out_specs=[SMEM, SMEM] + [VMEM] * groups,
        scratch_shapes=[
            pltpu.VMEM(integrals.shape, bf16),
            pltpu.SMEM((groups,), i32),
            pltpu.SemaphoreType.DMA,
        ],
        cost_estimate=cost(tasks * width * width, 2 * integrals.size),
        **params("first"),
    )(task_plan.T, integrals)
    order, labels, sent = outs[0], outs[1], list(outs[2:])
    sent += pl.pallas_call(
        functools.partial(rest_body, groups, cap, widths[0], widths[1:]),
        out_shape=[b for b in bare[1:] for _ in range(groups)],
        in_specs=[SMEM, VMEM],
        out_specs=[VMEM] * (groups * (chunks - 1)),
        cost_estimate=cost(tasks * width * width, 2 * integrals.size),
        **params("rest"),
    )(order, integrals)
    labels = [labels[0]] + [swap(labels[k], "group", k) for k in range(1, groups)]
    pieces = [
        [sent[c * groups]]
        + [swap(sent[c * groups + k], "group", k) for k in range(1, groups)]
        for c in range(chunks)
    ]

    count = lines * tile_dev
    keeps, codes, results, owns = [], [], [], []

    def contract(c):
        piece = widths[c]
        token = owns[c - 2 : c - 1] if c >= 2 else []
        keep, send = pl.pallas_call(
            functools.partial(contract_body, groups, members, tile_dev),
            out_shape=[
                shape((count, piece, rows), f32),
                shape((count * piece + pad16(count), rows), i16),
            ],
            in_specs=[SMEM] * groups + [VMEM] * groups + [ANY] * (members + len(token)),
            out_specs=[VMEM] * 2,
            scratch_shapes=[
                pltpu.VMEM((tile_grp, width, rows), bf16),
                pltpu.VMEM((tile_grp, piece, rows), f32),
                pltpu.VMEM((pad16(count), rows), f32),
                pltpu.SemaphoreType.DMA((members,)),
            ],
            cost_estimate=cost(2 * tasks * width * piece * rows, 8 << 20),
            **params("contract"),
        )(*labels, *pieces[c], *blocks, *token)
        keeps.append(keep)
        codes.append(swap(send, "member", 1))

    def middle(c):
        piece = widths[c]
        token = keeps[c + 1 : c + 2]
        out = pl.pallas_call(
            functools.partial(middle_body, lines, tile_dev),
            out_shape=[shape((tile_dev, piece, rows), f32)]
            + [shape((tile_dev * piece + pad16(tile_dev), rows), i16)] * (lines - 1),
            in_specs=[VMEM] * 2 + [ANY] * len(token),
            out_specs=[VMEM] * lines,
            scratch_shapes=[
                pltpu.VMEM((pad16(count), rows), f32),
                pltpu.VMEM((pad16(tile_dev), rows), f32),
            ],
            cost_estimate=cost(count * piece * rows * 20, 4 << 20),
            **params("middle"),
        )(keeps[c], codes[c], *token)
        owns.append(out[0])
        results.append(out[0])
        results.extend(swap(out[k], "member", 2 * k) for k in range(1, lines))

    contract(0)
    for c in range(1, chunks):
        contract(c)
        middle(c - 1)
    middle(chunks - 1)
    return pl.pallas_call(
        functools.partial(last_body, chunks, lines, tile_dev),
        out_shape=shape((tile_dev, rows, width), f32),
        in_specs=[VMEM] * len(results),
        out_specs=VMEM,
        scratch_shapes=[
            pltpu.VMEM((lines - 1, pad16(tile_dev), rows), f32),
            pltpu.VMEM((tile_dev, width, rows), f32),
        ],
        cost_estimate=cost(tile_dev * width * rows * 20, 4 << 20),
        **params("last"),
    )(*results)


def solution(mesh):
    in_specs = (
        P(("group", "member"), None, None),
        P(("group", "member"), None, None),
        P(("group", "member"), None),
    )
    out_specs = P(("group", "member"), None, None)

    return jax.shard_map(on_device, mesh=mesh, in_specs=in_specs, out_specs=out_specs, check_vma=False)
```
